128 devices in a mesh: sector: 16 (over z_lo, y, core), op: 8 (over x, z_hi).
Axes of the slice: x: 4, y: 4, z: 4 (z_hi: 2, z_lo: 2; z = z_hi * 2 + z_lo), core: 2. Of those that a mesh axis runs over, the one named last changes fastest.
Arguments:
- wavefunction: bfloat16 [16, 768, 1536], P('sector', 'op'), may hold values from -6 to 6
- basis: bfloat16 [16, 1536, 768], P('sector'), may hold values from -0.15625 to 0.15625
- left_ops: bfloat16 [40, 768, 768], P('op'), may hold values from -0.03125 to 0.03125
- right_ops: bfloat16 [40, 768, 768], P('op'), may hold values from -0.21875 to 0.21875
- offsets: int32 [40], P('op'), may hold values from -2 to 2, as said below
- sector_sizes: int32 [16], P('sector'), may hold values from 384 to 1536
Outputs:
- evolved: bfloat16 [16, 768, 1536], P('sector', 'op')
The draws below stay inside these ranges and needn't reach their ends.
Inputs may be any that keep to these rules, and one draw needn't show every extreme that they name: Every value from -2 to 2 occurs among the 40 offsets, any two of them equally often up to one. Only the first sector_sizes[s] left states of sector s are live.
All inputs are finite; a program needn't handle non-finite values.
Results may differ from the reference program's by a relative error of at most 0.014.
Values may be sent and summed in bfloat16 or wider, within the bound.
A program may use at most 128 MiB of HBM per device.

```python
import jax
import jax.numpy as jnp
from jax import lax

BOND = 768
LEFT = 1536
REACH = 2
STEPS = 2
SECTORS = 16
PAIRS = 40


def draw_offsets(key, part):
    ordering = jax.random.permutation(jax.random.fold_in(key, 11), PAIRS)
    return (ordering % (2 * REACH + 1) - REACH).astype(jnp.int32)


def with_ends(array, rng, low, high):
    dims = array.shape
    place = [jax.random.randint(jax.random.fold_in(rng, axis), (), 0, dims[axis]) for axis in range(len(dims))]
    array = array.at[tuple(place)].set(low)
    longest = dims.index(max(dims))
    place[longest] = (place[longest] + 1) % dims[longest]
    return array.at[tuple(place)].set(high)


def block_scale(key, shape, shards, least, high):
    factor_of, own = 1.0, jax.random.fold_in(key, 6)
    for dim, shards_of in shards:
        steps = jnp.exp(jax.random.uniform(jax.random.fold_in(own, dim), (shards_of,), jnp.float32, least / len(shards), high / len(shards)))
        factor_of = factor_of * jnp.repeat(steps, shape[dim] // shards_of).reshape([-1 if axis == dim else 1 for axis in range(len(shape))])
    return factor_of


def centred(stream_key, shape, scale, most, split=(), held_as=jnp.bfloat16):
    entries = jax.random.normal(stream_key, shape, jnp.float32) * scale
    if len(split) > 0:
        entries = block_scale(stream_key, shape, split, -0.22, 0.18) * entries
    return jnp.clip(entries, min=-most, max=most).astype(held_as)


def setup_inputs(seed: int = 0) -> dict:
    streams_of = jax.random.split(jax.random.key(seed), 7)
    wavefunction = centred(streams_of[0], (SECTORS, BOND, LEFT), 1.0, 6.0, ((0, 16), (1, 8)))
    basis = centred(streams_of[1], (SECTORS, LEFT, BOND), LEFT ** -0.5, 0.15625, ((0, 16),))
    left_ops = centred(streams_of[2], (PAIRS, BOND, BOND), (BOND * PAIRS) ** -0.5, 0.03125, ((0, 8),))
    right_ops = centred(streams_of[3], (PAIRS, BOND, BOND), BOND ** -0.5, 0.21875, ((0, 8),))
    offsets = draw_offsets(jax.random.fold_in(streams_of[6], 71), 0)
    sector_sizes = with_ends(jax.random.randint(streams_of[5], (SECTORS,), LEFT // 4, LEFT + 1), jax.random.fold_in(streams_of[5], 1), LEFT // 4, LEFT).astype(jnp.int32)
    return {"wavefunction": wavefunction, "basis": basis, "left_ops": left_ops, "right_ops": right_ops, "offsets": offsets, "sector_sizes": sector_sizes}


increment_width = 0.75


def reference(wavefunction, basis, left_ops, right_ops, offsets, sector_sizes):
    sector_count = wavefunction.shape[0]
    column_entries = jnp.arange(wavefunction.shape[2], dtype=jnp.int32)
    live_mask = column_entries[None, :] < sector_sizes[:, None]
    current = jnp.where(live_mask[:, None, :], wavefunction, jnp.zeros_like(wavefunction))
    masked_basis = jnp.where(live_mask[:, :, None], basis, jnp.zeros_like(basis))
    sector_ids = jnp.arange(sector_count, dtype=jnp.int32)
    left_wide = left_ops.astype(jnp.float32)
    broad_east_factor = right_ops.astype(jnp.float32)
    enlarged_state_space = masked_basis.astype(jnp.float32)
    for repeat in range(STEPS):
        transformed_blocks = jnp.einsum("sbl,slc->sbc", current.astype(jnp.float32), enlarged_state_space).astype(jnp.bfloat16)
        transformed_blocks = lax.optimization_barrier(transformed_blocks)

        def single_sector(sector_index):
            targets = (sector_index + offsets).astype(jnp.int32)
            inside_range = (targets >= 0) & (targets < sector_count)
            guarded_destinations = jnp.clip(targets, 0, sector_count - 1).astype(jnp.int32)
            chosen_tiles = transformed_blocks[guarded_destinations]
            chosen_tiles = jnp.where(inside_range[:, None, None], chosen_tiles, jnp.zeros_like(chosen_tiles))
            half_product = jnp.einsum("kab,kbc->kac", left_wide, chosen_tiles.astype(jnp.float32)).astype(jnp.bfloat16)
            half_product = lax.optimization_barrier(half_product)
            return jnp.einsum("kac,kdc->ad", half_product.astype(jnp.float32), broad_east_factor)

        overall_tile_count = lax.map(single_sector, sector_ids).astype(jnp.bfloat16)
        overall_tile_count = lax.optimization_barrier(overall_tile_count)
        lifted_tiles = jnp.einsum("zqt,zit->zqi", overall_tile_count.astype(jnp.float32), enlarged_state_space)
        current = (current.astype(jnp.float32) - increment_width * lifted_tiles).astype(jnp.bfloat16)
    return current
```

```python
import functools

import jax
import jax.numpy as jnp
from jax import lax
from jax.experimental import pallas as pl
from jax.experimental.pallas import tpu as pltpu
from jax.sharding import PartitionSpec as P

BOND = 768
LEFT = 1536
REACH = 2
STEPS = 2
PER = 5
ROWS = 96
CW = 256
CHUNKS = BOND // CW
OPS = 8
increment_width = 0.75
MESH = pl.DeviceIdType.MESH
METHOD = ("B", "B", "N")
ORDER = (0, 2, 1)


def dot_nt(a, b):
    return lax.dot_general(
        a, b, (((1,), (1,)), ((), ())), preferred_element_type=jnp.float32
    )


def dot_nn(a, b):
    return jnp.dot(a, b, preferred_element_type=jnp.float32)


class Names:
    def __init__(self):
        self.index = {}

    def __call__(self, *key):
        return self.index.setdefault(key, len(self.index))


SEMS = 80


def kernel(
    off_ref, size_ref, wf_hbm, basis_hbm, left_hbm, right_hbm, out_ref,
    left, right, basis, cur, x00, x01, x02, x10, x11, x12,
    h, acc, part, arrived, send_sem, recv_sem, rs_send, rs_recv, load_sem,
):
    s = lax.axis_index("sector")
    o = lax.axis_index("op")
    x, zh = o // 2, lax.rem(o, 2)
    core = lax.rem(s, 2)
    chip = s // 2
    has_lo, has_hi = chip > 0, chip < 7
    partner = s + 1 - 2 * core
    z_peer = x * 2 + (1 - zh)
    x_right = lax.rem(x + 1, 4)
    x_left = lax.rem(x + 3, 4)
    x_far = lax.rem(x + 2, 4)
    op_right, op_left = x_right * 2 + zh, x_left * 2 + zh

    loads = {}

    def load(name, src, dst, i):
        cp = pltpu.make_async_copy(src, dst, load_sem.at[i])
        cp.start()
        loads[name] = cp

    load("wf", wf_hbm.at[0], cur, 0)
    load("basis", basis_hbm.at[0], basis, 1)

    barrier = pltpu.get_barrier_semaphore()
    for j in range(1, OPS):
        pl.semaphore_signal(
            barrier, inc=1, device_id={"sector": s, "op": lax.rem(o + j, OPS)}, device_id_type=MESH
        )
    pl.semaphore_signal(barrier, inc=1, device_id={"sector": partner, "op": o}, device_id_type=MESH)

    @pl.when(has_lo)
    def _():
        pl.semaphore_signal(barrier, inc=1, device_id={"sector": s - 2, "op": o}, device_id_type=MESH)

    @pl.when(has_hi)
    def _():
        pl.semaphore_signal(barrier, inc=1, device_id={"sector": s + 2, "op": o}, device_id_type=MESH)

    load("left", left_hbm, left, 2)
    load("right", right_hbm, right, 3)

    xg = ((x00, x01, x02), (x10, x11, x12))

    for bufs in xg:
        for buf in bufs:
            @pl.when(jnp.logical_not(has_lo))
            def _():
                buf[0] = jnp.zeros((BOND, CW), jnp.bfloat16)

            @pl.when(jnp.logical_not(has_lo) & (core == 0))
            def _():
                buf[1] = jnp.zeros((BOND, CW), jnp.bfloat16)

            @pl.when(jnp.logical_not(has_hi))
            def _():
                buf[4] = jnp.zeros((BOND, CW), jnp.bfloat16)

            @pl.when(jnp.logical_not(has_hi) & (core == 1))
            def _():
                buf[3] = jnp.zeros((BOND, CW), jnp.bfloat16)

    columns = lax.broadcasted_iota(jnp.int32, (ROWS, LEFT), 1)
    live = columns < size_ref[0]
    loads["wf"].wait()
    cur[...] = jnp.where(live, cur[...], jnp.zeros((ROWS, LEFT), jnp.bfloat16))
    loads["basis"].wait()

    def rows_of(start, count):
        return pl.ds(pl.multiple_of(start, ROWS), count)

    own_rows = rows_of(o * ROWS, ROWS)
    z_rows = rows_of(z_peer * ROWS, ROWS)
    pair_rows = rows_of(x * 192, 192)
    left_pair = rows_of(x_left * 192, 192)
    right_pair = rows_of(x_right * 192, 192)
    far_pair = rows_of(x_far * 192, 192)
    lo_half = lambda px: rows_of(px * 192, ROWS)
    hi_half = lambda px: rows_of(px * 192 + ROWS, ROWS)

    for step in range(STEPS):
        names = Names()
        waits = []
        bufs = xg[step]

        def send(key, src, dst, sector, op, when=None):
            i = names(*key)

            def copy():
                return pltpu.make_async_remote_copy(
                    src_ref=src, dst_ref=dst,
                    send_sem=send_sem.at[step, i], recv_sem=recv_sem.at[step, i],
                    device_id={"sector": sector, "op": op}, device_id_type=MESH,
                )

            if when is None:
                copy().start()
            else:
                @pl.when(when)
                def _():
                    copy().start()
            waits.append((copy, when))

        def arrive(key, dst, when=None):
            i = names(*key)

            def body():
                pltpu.make_async_remote_copy(
                    src_ref=dst, dst_ref=dst,
                    send_sem=send_sem.at[step, i], recv_sem=recv_sem.at[step, i],
                    device_id={"sector": partner, "op": o}, device_id_type=MESH,
                ).wait_recv()

            if when is None:
                body()
            else:
                pl.when(when)(body)

        def slot_when(slot):
            return {0: has_lo, 2: None, 4: has_hi}[slot]

        def send_y(ch, rows, name):
            buf = bufs[ch]
            send((ch, "y-up", name), buf.at[2, rows], buf.at[0, rows], s + 2, o, has_hi)
            send((ch, "y-dn", name), buf.at[2, rows], buf.at[4, rows], s - 2, o, has_lo)

        def arrive_y(ch, rows, name):
            buf = bufs[ch]
            arrive((ch, "y-up", name), buf.at[0, rows], has_lo)
            arrive((ch, "y-dn", name), buf.at[4, rows], has_hi)

        def gather_z(ch, slot):
            buf = bufs[ch]
            send((ch, slot, "z"), buf.at[slot, own_rows], buf.at[slot, own_rows], s, z_peer, slot_when(slot))

        def gather_x(ch, slot):
            buf = bufs[ch]
            arrive((ch, slot, "z"), buf.at[slot, z_rows], slot_when(slot))
            pair = buf.at[slot, pair_rows]
            send((ch, slot, "right"), pair, pair, s, op_right, slot_when(slot))
            send((ch, slot, "left"), pair, pair, s, op_left, slot_when(slot))

        def relay_x(ch, slot):
            buf = bufs[ch]
            arrive((ch, slot, "right"), buf.at[slot, left_pair], slot_when(slot))
            half = buf.at[slot, lo_half(x_left)]
            send((ch, slot, "right2"), half, half, s, op_right, slot_when(slot))
            arrive((ch, slot, "left"), buf.at[slot, right_pair], slot_when(slot))
            half = buf.at[slot, hi_half(x_right)]
            send((ch, slot, "left2"), half, half, s, op_left, slot_when(slot))

        def finish_x(ch, slot):
            buf = bufs[ch]
            arrive((ch, slot, "right2"), buf.at[slot, lo_half(x_far)], slot_when(slot))
            arrive((ch, slot, "left2"), buf.at[slot, hi_half(x_far)], slot_when(slot))

        def own_across(ch):
            buf = bufs[ch]
            send((ch, "own"), buf.at[2], buf.at[1 + 2 * core], partner, o)

        def far_across(ch):
            buf = bufs[ch]
            there = ((core == 0) & has_hi) | ((core == 1) & has_lo)
            send((ch, "far"), buf.at[4 - 4 * core], buf.at[3 - 2 * core], partner, o, there)

        def arrive_across(ch):
            buf = bufs[ch]
            here = ((core == 0) & has_lo) | ((core == 1) & has_hi)
            arrive((ch, "own"), buf.at[3 - 2 * core])
            arrive((ch, "far"), buf.at[1 + 2 * core], here)

        def halves(ch):
            buf = bufs[ch]

            def body(k, carry):
                d = off_ref[k] + REACH
                h[k] = dot_nn(left[k], buf[d]).astype(jnp.bfloat16)
                return carry

            lax.fori_loop(0, PER, body, 0)

        def second(ch, rows):
            total = None
            for k in range(PER):
                term = dot_nt(h[k, rows], right[k, :, ch * CW : (ch + 1) * CW])
                total = term if total is None else total + term
            return total

        def accumulate(ch, first):
            def body(i, carry):
                rows = pl.ds(pl.multiple_of(i * 384, 384), 384)
                if first:
                    acc[rows] = second(ch, rows)
                else:
                    acc[rows] += second(ch, rows)
                return carry

            lax.fori_loop(0, 2, body, 0)

        rotated = dot_nn(cur[...], basis[...]).astype(jnp.bfloat16)
        for ch in range(CHUNKS):
            bufs[ch][2, own_rows] = rotated[:, ch * CW : (ch + 1) * CW]
        if step == 0:
            pl.semaphore_wait(
                barrier, OPS + has_lo.astype(jnp.int32) + has_hi.astype(jnp.int32)
            )

        blocks = [ch for ch in range(CHUNKS) if METHOD[ch] == "B"]
        early = [ch for ch in range(CHUNKS) if METHOD[ch] == "N"]
        for ch in blocks:
            gather_z(ch, 2)
        for ch in early:
            send_y(ch, own_rows, "rows")
            gather_z(ch, 2)
        for ch in blocks:
            gather_x(ch, 2)
            send_y(ch, pair_rows, "pair")
        for ch in early:
            arrive_y(ch, own_rows, "rows")
            gather_z(ch, 0)
            gather_z(ch, 4)
            gather_x(ch, 2)
        for ch in blocks:
            relay_x(ch, 2)
            send_y(ch, left_pair, "left")
            send_y(ch, right_pair, "right")
        for ch in early:
            gather_x(ch, 0)
            gather_x(ch, 4)
            relay_x(ch, 2)
        for ch in blocks:
            finish_x(ch, 2)
            send_y(ch, far_pair, "far")
            own_across(ch)
        for ch in early:
            finish_x(ch, 2)
            own_across(ch)
            relay_x(ch, 0)
            relay_x(ch, 4)

        if step == 0:
            loads["left"].wait()
            loads["right"].wait()

        for n, ch in enumerate(ORDER):
            if METHOD[ch] == "B":
                arrive_y(ch, pair_rows, "pair")
                arrive_y(ch, right_pair, "left")
                arrive_y(ch, left_pair, "right")
                arrive_y(ch, far_pair, "far")
            else:
                finish_x(ch, 0)
                finish_x(ch, 4)
            far_across(ch)
            arrive_across(ch)
            halves(ch)
            if n < CHUNKS - 1:
                accumulate(ch, n == 0)
        last = ORDER[-1]
        rs_waits = []
        for i in range(2):
            half = lax.rem(x // 2 + 1 + i, 2)
            rows = pl.ds(pl.multiple_of(half * 384, 384), 384)
            part[step, rows] = (acc[rows] + second(last, rows)).astype(jnp.bfloat16)
            for j in range(4):
                peer = half * 4 + lax.rem(lax.rem(o, 4) + 3 - j, 4)
                peer_rows = rows_of(peer * ROWS, ROWS)

                def copy(peer=peer, peer_rows=peer_rows):
                    return pltpu.make_async_remote_copy(
                        src_ref=part.at[step, peer_rows], dst_ref=arrived.at[step, o],
                        send_sem=rs_send.at[step, peer], recv_sem=rs_recv.at[step, o],
                        device_id={"sector": s, "op": peer}, device_id_type=MESH,
                    )

                if i == 1 and j == 3:
                    continue
                copy().start()
                rs_waits.append(copy)

        total = part[step, own_rows].astype(jnp.float32)
        for j in range(1, OPS):
            peer = lax.rem(o + j, OPS)
            pltpu.make_async_remote_copy(
                src_ref=arrived.at[step, peer], dst_ref=arrived.at[step, peer],
                send_sem=rs_send.at[step, peer], recv_sem=rs_recv.at[step, peer],
                device_id={"sector": s, "op": peer}, device_id_type=MESH,
            ).wait_recv()
            total = total + arrived[step, peer].astype(jnp.float32)
        summed = total.astype(jnp.bfloat16)
        lifted = dot_nt(summed, basis[...])
        fresh = (cur[...].astype(jnp.float32) - increment_width * lifted).astype(jnp.bfloat16)
        fresh = jnp.where(live, fresh, jnp.zeros_like(fresh))
        if step == STEPS - 1:
            out_ref[0] = fresh
        else:
            cur[...] = fresh
        for copy in rs_waits:
            copy().wait_send()
        for copy, when in waits:
            if when is None:
                copy().wait_send()
            else:
                @pl.when(when)
                def _():
                    copy().wait_send()
        assert len(names.index) <= SEMS


def on_device(wavefunction, basis, left_ops, right_ops, offsets, sector_sizes):
    any_space = pl.BlockSpec(memory_space=pl.ANY)
    smem = pl.BlockSpec(memory_space=pltpu.SMEM)
    block = pltpu.VMEM((2 * REACH + 1, BOND, CW), jnp.bfloat16)
    return pl.pallas_call(
        kernel,
        out_shape=jax.ShapeDtypeStruct((1, ROWS, LEFT), jnp.bfloat16),
        in_specs=[smem, smem, any_space, any_space, any_space, any_space],
        out_specs=pl.BlockSpec(memory_space=pltpu.VMEM),
        scratch_shapes=[
            pltpu.VMEM((PER, BOND, BOND), jnp.bfloat16),
            pltpu.VMEM((PER, BOND, BOND), jnp.bfloat16),
            pltpu.VMEM((LEFT, BOND), jnp.bfloat16),
            pltpu.VMEM((ROWS, LEFT), jnp.bfloat16),
            block, block, block, block, block, block,
            pltpu.VMEM((PER, BOND, CW), jnp.bfloat16),
            pltpu.VMEM((BOND, BOND), jnp.float32),
            pltpu.VMEM((STEPS, BOND, BOND), jnp.bfloat16),
            pltpu.VMEM((STEPS, OPS, ROWS, BOND), jnp.bfloat16),
            pltpu.SemaphoreType.DMA((STEPS, SEMS)),
            pltpu.SemaphoreType.DMA((STEPS, SEMS)),
            pltpu.SemaphoreType.DMA((STEPS, OPS)),
            pltpu.SemaphoreType.DMA((STEPS, OPS)),
            pltpu.SemaphoreType.DMA((4,)),
        ],
        compiler_params=pltpu.CompilerParams(
            collective_id=0, has_side_effects=True, vmem_limit_bytes=62 * 1024 * 1024
        ),
        name="hamiltonian",
    )(offsets, sector_sizes, wavefunction, basis, left_ops, right_ops)


def solution(mesh):
    return jax.shard_map(
        on_device,
        mesh=mesh,
        in_specs=(
            P("sector", "op", None),
            P("sector", None, None),
            P("op", None, None),
            P("op", None, None),
            P("op"),
            P("sector"),
        ),
        out_specs=P("sector", "op", None),
        check_vma=False,
    )
```

```python
import functools

import jax
import jax.numpy as jnp
from jax import lax
from jax.experimental import pallas as pl
from jax.experimental.pallas import tpu as pltpu
from jax.sharding import PartitionSpec as P

BOND = 768
LEFT = 1536
REACH = 2
STEPS = 2
PER = 5
ROWS = 96
CW = 256
CHUNKS = BOND // CW
OPS = 8
increment_width = 0.75
MESH = pl.DeviceIdType.MESH
METHOD = ("B", "B", "N")
ORDER = (0, 2, 1)


def dot_nt(a, b):
    return lax.dot_general(
        a, b, (((1,), (1,)), ((), ())), preferred_element_type=jnp.float32
    )


def dot_nn(a, b):
    return jnp.dot(a, b, preferred_element_type=jnp.float32)


class Names:
    def __init__(self):
        self.index = {}

    def __call__(self, *key):
        return self.index.setdefault(key, len(self.index))


SEMS = 80


def kernel(
    off_ref, size_ref, wf_hbm, basis_hbm, left_hbm, right_hbm, out_ref,
    left, right, basis, cur, x00, x01, x02, x10, x11, x12,
    h, acc, part, arrived, send_sem, recv_sem, rs_send, rs_recv, load_sem,
):
    s = lax.axis_index("sector")
    o = lax.axis_index("op")
    x, zh = o // 2, lax.rem(o, 2)
    core = lax.rem(s, 2)
    chip = s // 2
    has_lo, has_hi = chip > 0, chip < 7
    cross_lo, cross_hi = chip == 4, chip == 3
    plain_lo, plain_hi = has_lo & (chip != 4), has_hi & (chip != 3)
    partner = s + 1 - 2 * core
    z_peer = x * 2 + (1 - zh)
    x_right = lax.rem(x + 1, 4)
    x_left = lax.rem(x + 3, 4)
    x_far = lax.rem(x + 2, 4)
    op_right, op_left = x_right * 2 + zh, x_left * 2 + zh

    loads = {}

    def load(name, src, dst, i):
        cp = pltpu.make_async_copy(src, dst, load_sem.at[i])
        cp.start()
        loads[name] = cp

    load("wf", wf_hbm.at[0], cur, 0)
    load("basis", basis_hbm.at[0], basis, 1)

    barrier = pltpu.get_barrier_semaphore()
    for j in range(1, OPS):
        pl.semaphore_signal(
            barrier, inc=1, device_id={"sector": s, "op": lax.rem(o + j, OPS)}, device_id_type=MESH
        )
    pl.semaphore_signal(barrier, inc=1, device_id={"sector": partner, "op": o}, device_id_type=MESH)

    @pl.when(has_lo)
    def _():
        pl.semaphore_signal(barrier, inc=1, device_id={"sector": s - 2, "op": o}, device_id_type=MESH)

    @pl.when(has_hi)
    def _():
        pl.semaphore_signal(barrier, inc=1, device_id={"sector": s + 2, "op": o}, device_id_type=MESH)

    load("left", left_hbm, left, 2)
    load("right", right_hbm, right, 3)

    xg = ((x00, x01, x02), (x10, x11, x12))

    def blank(bufs):
        for buf in bufs:
            @pl.when(jnp.logical_not(has_lo))
            def _():
                buf[0] = jnp.zeros((BOND, CW), jnp.bfloat16)

            @pl.when(jnp.logical_not(has_lo) & (core == 0))
            def _():
                buf[1] = jnp.zeros((BOND, CW), jnp.bfloat16)

            @pl.when(jnp.logical_not(has_hi))
            def _():
                buf[4] = jnp.zeros((BOND, CW), jnp.bfloat16)

            @pl.when(jnp.logical_not(has_hi) & (core == 1))
            def _():
                buf[3] = jnp.zeros((BOND, CW), jnp.bfloat16)

    columns = lax.broadcasted_iota(jnp.int32, (ROWS, LEFT), 1)
    live = columns < size_ref[0]
    loads["wf"].wait()
    cur[...] = jnp.where(live, cur[...], jnp.zeros((ROWS, LEFT), jnp.bfloat16))
    loads["basis"].wait()

    def rows_of(start, count):
        return pl.ds(pl.multiple_of(start, ROWS), count)

    own_rows = rows_of(o * ROWS, ROWS)
    z_rows = rows_of(z_peer * ROWS, ROWS)
    pair_rows = rows_of(x * 192, 192)
    left_pair = rows_of(x_left * 192, 192)
    right_pair = rows_of(x_right * 192, 192)
    far_pair = rows_of(x_far * 192, 192)
    lo_half = lambda px: rows_of(px * 192, ROWS)
    hi_half = lambda px: rows_of(px * 192 + ROWS, ROWS)

    for step in range(STEPS):
        names = Names()
        waits = []
        bufs = xg[step]

        def send(key, src, dst, sector, op, when=None):
            i = names(*key)

            def copy():
                return pltpu.make_async_remote_copy(
                    src_ref=src, dst_ref=dst,
                    send_sem=send_sem.at[step, i], recv_sem=recv_sem.at[step, i],
                    device_id={"sector": sector, "op": op}, device_id_type=MESH,
                )

            if when is None:
                copy().start()
            else:
                @pl.when(when)
                def _():
                    copy().start()
            waits.append((copy, when))

        def arrive(key, dst, when=None):
            i = names(*key)

            def body():
                pltpu.make_async_remote_copy(
                    src_ref=dst, dst_ref=dst,
                    send_sem=send_sem.at[step, i], recv_sem=recv_sem.at[step, i],
                    device_id={"sector": partner, "op": o}, device_id_type=MESH,
                ).wait_recv()

            if when is None:
                body()
            else:
                pl.when(when)(body)

        def slot_when(slot):
            return {0: has_lo, 2: None, 4: has_hi}[slot]

        def send_y(ch, rows, name, up=has_hi, down=has_lo):
            buf = bufs[ch]
            send((ch, "y-up", name), buf.at[2, rows], buf.at[0, rows], s + 2, o, up)
            send((ch, "y-dn", name), buf.at[2, rows], buf.at[4, rows], s - 2, o, down)

        def arrive_y(ch, rows, name):
            buf = bufs[ch]
            arrive((ch, "y-up", name), buf.at[0, rows], has_lo)
            arrive((ch, "y-dn", name), buf.at[4, rows], has_hi)

        def gather_z(ch, slot):
            buf = bufs[ch]
            send((ch, slot, "z"), buf.at[slot, own_rows], buf.at[slot, own_rows], s, z_peer, slot_when(slot))

        def arrive_z(ch, slot):
            arrive((ch, slot, "z"), bufs[ch].at[slot, z_rows], slot_when(slot))

        def gather_x(ch, slot):
            buf = bufs[ch]
            pair = buf.at[slot, pair_rows]
            send((ch, slot, "right"), pair, pair, s, op_right, slot_when(slot))
            send((ch, slot, "left"), pair, pair, s, op_left, slot_when(slot))

        def relay_x(ch, slot):
            buf = bufs[ch]
            arrive((ch, slot, "right"), buf.at[slot, left_pair], slot_when(slot))
            half = buf.at[slot, lo_half(x_left)]
            send((ch, slot, "right2"), half, half, s, op_right, slot_when(slot))
            arrive((ch, slot, "left"), buf.at[slot, right_pair], slot_when(slot))
            half = buf.at[slot, hi_half(x_right)]
            send((ch, slot, "left2"), half, half, s, op_left, slot_when(slot))

        def finish_x(ch, slot):
            buf = bufs[ch]
            arrive((ch, slot, "right2"), buf.at[slot, lo_half(x_far)], slot_when(slot))
            arrive((ch, slot, "left2"), buf.at[slot, hi_half(x_far)], slot_when(slot))

        def own_across(ch):
            buf = bufs[ch]
            send((ch, "own"), buf.at[2], buf.at[1 + 2 * core], partner, o)

        def far_across(ch):
            buf = bufs[ch]
            there = ((core == 0) & has_hi) | ((core == 1) & has_lo)
            send((ch, "far"), buf.at[4 - 4 * core], buf.at[3 - 2 * core], partner, o, there)

        def arrive_across(ch):
            buf = bufs[ch]
            here = ((core == 0) & has_lo) | ((core == 1) & has_hi)
            arrive((ch, "own"), buf.at[3 - 2 * core])
            arrive((ch, "far"), buf.at[1 + 2 * core], here)

        def halves(ch):
            buf = bufs[ch]

            def body(k, carry):
                d = off_ref[k] + REACH
                h[k] = dot_nn(left[k], buf[d]).astype(jnp.bfloat16)
                return carry

            lax.fori_loop(0, PER, body, 0)

        def second(ch, rows):
            total = None
            for k in range(PER):
                term = dot_nt(h[k, rows], right[k, :, ch * CW : (ch + 1) * CW])
                total = term if total is None else total + term
            return total

        def accumulate(ch, first):
            def body(i, carry):
                rows = pl.ds(pl.multiple_of(i * 384, 384), 384)
                if first:
                    acc[rows] = second(ch, rows)
                else:
                    acc[rows] += second(ch, rows)
                return carry

            lax.fori_loop(0, 2, body, 0)

        rotated = dot_nn(cur[...], basis[...]).astype(jnp.bfloat16)
        for ch in range(CHUNKS):
            bufs[ch][2, own_rows] = rotated[:, ch * CW : (ch + 1) * CW]
        if step == 0:
            pl.semaphore_wait(
                barrier, OPS + has_lo.astype(jnp.int32) + has_hi.astype(jnp.int32)
            )

        a, b, d = 0, 1, 2
        gather_z(a, 2)
        gather_z(d, 2)
        gather_z(b, 2)
        if step == 0:
            blank(xg[0])
            blank(xg[1])
        arrive_z(a, 2)
        gather_x(a, 2)
        send_y(a, pair_rows, "pair", plain_hi, plain_lo)
        arrive_z(d, 2)
        send_y(d, pair_rows, "pair")
        arrive_z(b, 2)
        gather_x(b, 2)
        gather_x(d, 2)
        relay_x(a, 2)
        send_y(a, pair_rows, "pair", cross_hi, cross_lo)
        send_y(a, left_pair, "left")
        send_y(a, right_pair, "right")
        arrive_y(d, pair_rows, "pair")
        gather_x(d, 0)
        gather_x(d, 4)
        finish_x(a, 2)
        send_y(a, far_pair, "far")
        own_across(a)
        relay_x(b, 2)
        send_y(b, pair_rows, "pair")
        send_y(b, left_pair, "left")
        send_y(b, right_pair, "right")
        relay_x(d, 2)
        finish_x(b, 2)
        send_y(b, far_pair, "far")
        own_across(b)
        finish_x(d, 2)
        own_across(d)
        relay_x(d, 0)
        relay_x(d, 4)

        if step == 0:
            loads["left"].wait()
            loads["right"].wait()

        for n, ch in enumerate(ORDER):
            if METHOD[ch] == "B":
                arrive_y(ch, pair_rows, "pair")
                arrive_y(ch, left_pair, "left")
                arrive_y(ch, right_pair, "right")
                arrive_y(ch, far_pair, "far")
            else:
                finish_x(ch, 0)
                finish_x(ch, 4)
            far_across(ch)
            arrive_across(ch)
            halves(ch)
            if n < CHUNKS - 1:
                accumulate(ch, n == 0)
        last = ORDER[-1]
        rs_waits = []
        for i in range(2):
            half = lax.rem(x // 2 + 1 + i, 2)
            rows = pl.ds(pl.multiple_of(half * 384, 384), 384)
            part[step, rows] = (acc[rows] + second(last, rows)).astype(jnp.bfloat16)
            for j in range(4):
                peer = half * 4 + lax.rem(lax.rem(o, 4) + 3 - j, 4)
                peer_rows = rows_of(peer * ROWS, ROWS)

                def copy(peer=peer, peer_rows=peer_rows):
                    return pltpu.make_async_remote_copy(
                        src_ref=part.at[step, peer_rows], dst_ref=arrived.at[step, o],
                        send_sem=rs_send.at[step, peer], recv_sem=rs_recv.at[step, o],
                        device_id={"sector": s, "op": peer}, device_id_type=MESH,
                    )

                if i == 1 and j == 3:
                    continue
                copy().start()
                rs_waits.append(copy)

        total = part[step, own_rows].astype(jnp.float32)
        for j in range(1, OPS):
            peer = lax.rem(o + j, OPS)
            pltpu.make_async_remote_copy(
                src_ref=arrived.at[step, peer], dst_ref=arrived.at[step, peer],
                send_sem=rs_send.at[step, peer], recv_sem=rs_recv.at[step, peer],
                device_id={"sector": s, "op": peer}, device_id_type=MESH,
            ).wait_recv()
            total = total + arrived[step, peer].astype(jnp.float32)
        summed = total.astype(jnp.bfloat16)
        lifted = dot_nt(summed, basis[...])
        fresh = (cur[...].astype(jnp.float32) - increment_width * lifted).astype(jnp.bfloat16)
        fresh = jnp.where(live, fresh, jnp.zeros_like(fresh))
        if step == STEPS - 1:
            out_ref[0] = fresh
        else:
            cur[...] = fresh
        for copy in rs_waits:
            copy().wait_send()
        for copy, when in waits:
            if when is None:
                copy().wait_send()
            else:
                @pl.when(when)
                def _():
                    copy().wait_send()
        assert len(names.index) <= SEMS


def on_device(wavefunction, basis, left_ops, right_ops, offsets, sector_sizes):
    any_space = pl.BlockSpec(memory_space=pl.ANY)
    smem = pl.BlockSpec(memory_space=pltpu.SMEM)
    block = pltpu.VMEM((2 * REACH + 1, BOND, CW), jnp.bfloat16)
    return pl.pallas_call(
        kernel,
        out_shape=jax.ShapeDtypeStruct((1, ROWS, LEFT), jnp.bfloat16),
        in_specs=[smem, smem, any_space, any_space, any_space, any_space],
        out_specs=pl.BlockSpec(memory_space=pltpu.VMEM),
        scratch_shapes=[
            pltpu.VMEM((PER, BOND, BOND), jnp.bfloat16),
            pltpu.VMEM((PER, BOND, BOND), jnp.bfloat16),
            pltpu.VMEM((LEFT, BOND), jnp.bfloat16),
            pltpu.VMEM((ROWS, LEFT), jnp.bfloat16),
            block, block, block, block, block, block,
            pltpu.VMEM((PER, BOND, CW), jnp.bfloat16),
            pltpu.VMEM((BOND, BOND), jnp.float32),
            pltpu.VMEM((STEPS, BOND, BOND), jnp.bfloat16),
            pltpu.VMEM((STEPS, OPS, ROWS, BOND), jnp.bfloat16),
            pltpu.SemaphoreType.DMA((STEPS, SEMS)),
            pltpu.SemaphoreType.DMA((STEPS, SEMS)),
            pltpu.SemaphoreType.DMA((STEPS, OPS)),
            pltpu.SemaphoreType.DMA((STEPS, OPS)),
            pltpu.SemaphoreType.DMA((4,)),
        ],
        compiler_params=pltpu.CompilerParams(
            collective_id=0, has_side_effects=True, vmem_limit_bytes=62 * 1024 * 1024
        ),
        name="hamiltonian",
    )(offsets, sector_sizes, wavefunction, basis, left_ops, right_ops)


def solution(mesh):
    return jax.shard_map(
        on_device,
        mesh=mesh,
        in_specs=(
            P("sector", "op", None),
            P("sector", None, None),
            P("op", None, None),
            P("op", None, None),
            P("op"),
            P("sector"),
        ),
        out_specs=P("sector", "op", None),
        check_vma=False,
    )
```

```python
import functools

import jax
import jax.numpy as jnp
from jax import lax
from jax.experimental import pallas as pl
from jax.experimental.pallas import tpu as pltpu
from jax.sharding import PartitionSpec as P

BOND = 768
LEFT = 1536
REACH = 2
STEPS = 2
PER = 5
ROWS = 96
CW = 256
CHUNKS = BOND // CW
OPS = 8
increment_width = 0.75
MESH = pl.DeviceIdType.MESH
METHOD = ("B", "B", "N")
ORDER = (0, 2, 1)


def dot_nt(a, b):
    return lax.dot_general(
        a, b, (((1,), (1,)), ((), ())), preferred_element_type=jnp.float32
    )


def dot_nn(a, b):
    return jnp.dot(a, b, preferred_element_type=jnp.float32)


class Names:
    def __init__(self):
        self.index = {}

    def __call__(self, *key):
        return self.index.setdefault(key, len(self.index))


SEMS = 80


def kernel(
    off_ref, size_ref, wf_hbm, basis_hbm, left_hbm, right_hbm, out_ref,
    left, right, basis, cur, x00, x01, x02, x10, x11, x12,
    h, acc, part, arrived, send_sem, recv_sem, rs_send, rs_recv, load_sem,
):
    s = lax.axis_index("sector")
    o = lax.axis_index("op")
    x, zh = o // 2, lax.rem(o, 2)
    core = lax.rem(s, 2)
    chip = s // 2
    has_lo, has_hi = chip > 0, chip < 7
    cross_lo, cross_hi = chip == 4, chip == 3
    plain_lo, plain_hi = has_lo & (chip != 4), has_hi & (chip != 3)
    partner = s + 1 - 2 * core
    z_peer = x * 2 + (1 - zh)
    x_right = lax.rem(x + 1, 4)
    x_left = lax.rem(x + 3, 4)
    x_far = lax.rem(x + 2, 4)
    op_right, op_left = x_right * 2 + zh, x_left * 2 + zh

    loads = {}

    def load(name, src, dst, i):
        cp = pltpu.make_async_copy(src, dst, load_sem.at[i])
        cp.start()
        loads[name] = cp

    load("wf", wf_hbm.at[0], cur, 0)
    load("basis", basis_hbm.at[0], basis, 1)

    barrier = pltpu.get_barrier_semaphore()
    for j in range(1, OPS):
        pl.semaphore_signal(
            barrier, inc=1, device_id={"sector": s, "op": lax.rem(o + j, OPS)}, device_id_type=MESH
        )
    pl.semaphore_signal(barrier, inc=1, device_id={"sector": partner, "op": o}, device_id_type=MESH)

    @pl.when(has_lo)
    def _():
        pl.semaphore_signal(barrier, inc=1, device_id={"sector": s - 2, "op": o}, device_id_type=MESH)

    @pl.when(has_hi)
    def _():
        pl.semaphore_signal(barrier, inc=1, device_id={"sector": s + 2, "op": o}, device_id_type=MESH)

    load("left", left_hbm, left, 2)
    for c in range(CHUNKS):
        for k in range(PER):
            span = slice(c * CW, (c + 1) * CW)
            load(
                ("right", c, k), right_hbm.at[k, :, span], right.at[c, :, k * CW : (k + 1) * CW],
                3 + c * PER + k,
            )

    xg = ((x00, x01, x02), (x10, x11, x12))

    def blank(bufs):
        for buf in bufs:
            @pl.when(jnp.logical_not(has_lo))
            def _():
                buf[0] = jnp.zeros((BOND, CW), jnp.bfloat16)

            @pl.when(jnp.logical_not(has_lo) & (core == 0))
            def _():
                buf[1] = jnp.zeros((BOND, CW), jnp.bfloat16)

            @pl.when(jnp.logical_not(has_hi))
            def _():
                buf[4] = jnp.zeros((BOND, CW), jnp.bfloat16)

            @pl.when(jnp.logical_not(has_hi) & (core == 1))
            def _():
                buf[3] = jnp.zeros((BOND, CW), jnp.bfloat16)

    columns = lax.broadcasted_iota(jnp.int32, (ROWS, LEFT), 1)
    live = columns < size_ref[0]
    loads["wf"].wait()
    cur[...] = jnp.where(live, cur[...], jnp.zeros((ROWS, LEFT), jnp.bfloat16))
    loads["basis"].wait()

    def rows_of(start, count):
        return pl.ds(pl.multiple_of(start, ROWS), count)

    own_rows = rows_of(o * ROWS, ROWS)
    z_rows = rows_of(z_peer * ROWS, ROWS)
    pair_rows = rows_of(x * 192, 192)
    left_pair = rows_of(x_left * 192, 192)
    right_pair = rows_of(x_right * 192, 192)
    far_pair = rows_of(x_far * 192, 192)
    lo_half = lambda px: rows_of(px * 192, ROWS)
    hi_half = lambda px: rows_of(px * 192 + ROWS, ROWS)

    for step in range(STEPS):
        names = Names()
        waits = []
        bufs = xg[step]

        def send(key, src, dst, sector, op, when=None):
            i = names(*key)

            def copy():
                return pltpu.make_async_remote_copy(
                    src_ref=src, dst_ref=dst,
                    send_sem=send_sem.at[step, i], recv_sem=recv_sem.at[step, i],
                    device_id={"sector": sector, "op": op}, device_id_type=MESH,
                )

            if when is None:
                copy().start()
            else:
                @pl.when(when)
                def _():
                    copy().start()
            waits.append((copy, when))

        def arrive(key, dst, when=None):
            i = names(*key)

            def body():
                pltpu.make_async_remote_copy(
                    src_ref=dst, dst_ref=dst,
                    send_sem=send_sem.at[step, i], recv_sem=recv_sem.at[step, i],
                    device_id={"sector": partner, "op": o}, device_id_type=MESH,
                ).wait_recv()

            if when is None:
                body()
            else:
                pl.when(when)(body)

        def slot_when(slot):
            return {0: has_lo, 2: None, 4: has_hi}[slot]

        def send_y(ch, rows, name, up=has_hi, down=has_lo):
            buf = bufs[ch]
            send((ch, "y-up", name), buf.at[2, rows], buf.at[0, rows], s + 2, o, up)
            send((ch, "y-dn", name), buf.at[2, rows], buf.at[4, rows], s - 2, o, down)

        def arrive_y(ch, rows, name):
            buf = bufs[ch]
            arrive((ch, "y-up", name), buf.at[0, rows], has_lo)
            arrive((ch, "y-dn", name), buf.at[4, rows], has_hi)

        def gather_z(ch, slot):
            buf = bufs[ch]
            send((ch, slot, "z"), buf.at[slot, own_rows], buf.at[slot, own_rows], s, z_peer, slot_when(slot))

        def arrive_z(ch, slot):
            arrive((ch, slot, "z"), bufs[ch].at[slot, z_rows], slot_when(slot))

        def gather_x(ch, slot):
            buf = bufs[ch]
            pair = buf.at[slot, pair_rows]
            send((ch, slot, "right"), pair, pair, s, op_right, slot_when(slot))
            send((ch, slot, "left"), pair, pair, s, op_left, slot_when(slot))

        def relay_x(ch, slot):
            buf = bufs[ch]
            arrive((ch, slot, "right"), buf.at[slot, left_pair], slot_when(slot))
            half = buf.at[slot, lo_half(x_left)]
            send((ch, slot, "right2"), half, half, s, op_right, slot_when(slot))
            arrive((ch, slot, "left"), buf.at[slot, right_pair], slot_when(slot))
            half = buf.at[slot, hi_half(x_right)]
            send((ch, slot, "left2"), half, half, s, op_left, slot_when(slot))

        def finish_x(ch, slot):
            buf = bufs[ch]
            arrive((ch, slot, "right2"), buf.at[slot, lo_half(x_far)], slot_when(slot))
            arrive((ch, slot, "left2"), buf.at[slot, hi_half(x_far)], slot_when(slot))

        def own_across(ch):
            buf = bufs[ch]
            send((ch, "own"), buf.at[2], buf.at[1 + 2 * core], partner, o)

        def far_across(ch):
            buf = bufs[ch]
            there = ((core == 0) & has_hi) | ((core == 1) & has_lo)
            send((ch, "far"), buf.at[4 - 4 * core], buf.at[3 - 2 * core], partner, o, there)

        def arrive_across(ch):
            buf = bufs[ch]
            here = ((core == 0) & has_lo) | ((core == 1) & has_hi)
            arrive((ch, "own"), buf.at[3 - 2 * core])
            arrive((ch, "far"), buf.at[1 + 2 * core], here)

        def halves(ch):
            buf = bufs[ch]

            def body(k, carry):
                d = off_ref[k] + REACH
                span = pl.ds(pl.multiple_of(k * CW, CW), CW)
                h[:, span] = dot_nn(left[k], buf[d]).astype(jnp.bfloat16)
                return carry

            lax.fori_loop(0, PER, body, 0, unroll=True)

        def second(ch, rows):
            return dot_nt(h[rows], right[ch])

        def accumulate(ch, first):
            rows = slice(None)
            if first:
                acc[...] = second(ch, rows)
            else:
                acc[...] += second(ch, rows)

        rotated = dot_nn(cur[...], basis[...]).astype(jnp.bfloat16)
        for ch in range(CHUNKS):
            bufs[ch][2, own_rows] = rotated[:, ch * CW : (ch + 1) * CW]
        if step == 0:
            pl.semaphore_wait(
                barrier, OPS + has_lo.astype(jnp.int32) + has_hi.astype(jnp.int32)
            )

        def bring(ch):
            if METHOD[ch] == "B":
                arrive_y(ch, pair_rows, "pair")
                arrive_y(ch, left_pair, "left")
                arrive_y(ch, right_pair, "right")
                arrive_y(ch, far_pair, "far")
            else:
                finish_x(ch, 0)
                finish_x(ch, 4)
            far_across(ch)

        a, b, d = 0, 1, 2
        gather_z(a, 2)
        gather_z(d, 2)
        gather_z(b, 2)
        if step == 0:
            blank(xg[0])
            blank(xg[1])
        arrive_z(a, 2)
        gather_x(a, 2)
        send_y(a, pair_rows, "pair", plain_hi, plain_lo)
        arrive_z(d, 2)
        send_y(d, pair_rows, "pair")
        arrive_z(b, 2)
        gather_x(b, 2)
        gather_x(d, 2)
        relay_x(a, 2)
        send_y(a, pair_rows, "pair", cross_hi, cross_lo)
        send_y(a, left_pair, "left")
        send_y(a, right_pair, "right")
        arrive_y(d, pair_rows, "pair")
        gather_x(d, 0)
        gather_x(d, 4)
        finish_x(a, 2)
        send_y(a, far_pair, "far")
        own_across(a)
        relay_x(b, 2)
        send_y(b, pair_rows, "pair")
        send_y(b, left_pair, "left")
        send_y(b, right_pair, "right")
        relay_x(d, 2)
        finish_x(b, 2)
        send_y(b, far_pair, "far")
        own_across(b)
        finish_x(d, 2)
        own_across(d)
        relay_x(d, 0)
        relay_x(d, 4)

        if step == 0:
            loads["left"].wait()
            for c in range(CHUNKS):
                for k in range(PER):
                    loads["right", c, k].wait()

        bring(a)
        arrive_across(a)
        halves(a)
        accumulate(a, True)
        bring(d)
        arrive_across(d)
        halves(d)
        bring(b)
        accumulate(d, False)
        arrive_across(b)
        halves(b)
        last = ORDER[-1]
        rs_waits = []
        for i in range(2):
            half = lax.rem(x // 2 + 1 + i, 2)
            rows = pl.ds(pl.multiple_of(half * 384, 384), 384)
            part[step, rows] = (acc[rows] + second(last, rows)).astype(jnp.bfloat16)
            for j in (((1, 3, 2, 0), (1, 3, 2)))[i]:
                peer = half * 4 + lax.rem(lax.rem(o, 4) + j, 4)
                peer_rows = rows_of(peer * ROWS, ROWS)

                def copy(peer=peer, peer_rows=peer_rows):
                    return pltpu.make_async_remote_copy(
                        src_ref=part.at[step, peer_rows], dst_ref=arrived.at[step, o],
                        send_sem=rs_send.at[step, peer], recv_sem=rs_recv.at[step, o],
                        device_id={"sector": s, "op": peer}, device_id_type=MESH,
                    )

                if i == 1 and j == 0:
                    continue
                copy().start()
                rs_waits.append(copy)

        total = part[step, own_rows].astype(jnp.float32)
        for j in range(1, OPS):
            peer = lax.rem(o + j, OPS)
            pltpu.make_async_remote_copy(
                src_ref=arrived.at[step, peer], dst_ref=arrived.at[step, peer],
                send_sem=rs_send.at[step, peer], recv_sem=rs_recv.at[step, peer],
                device_id={"sector": s, "op": peer}, device_id_type=MESH,
            ).wait_recv()
            total = total + arrived[step, peer].astype(jnp.float32)
        summed = total.astype(jnp.bfloat16)
        lifted = dot_nt(summed, basis[...])
        fresh = (cur[...].astype(jnp.float32) - increment_width * lifted).astype(jnp.bfloat16)
        fresh = jnp.where(live, fresh, jnp.zeros_like(fresh))
        if step == STEPS - 1:
            out_ref[0] = fresh
        else:
            cur[...] = fresh
        for copy in rs_waits:
            copy().wait_send()
        for copy, when in waits:
            if when is None:
                copy().wait_send()
            else:
                @pl.when(when)
                def _():
                    copy().wait_send()
        assert len(names.index) <= SEMS


def on_device(wavefunction, basis, left_ops, right_ops, offsets, sector_sizes):
    any_space = pl.BlockSpec(memory_space=pl.ANY)
    smem = pl.BlockSpec(memory_space=pltpu.SMEM)
    block = pltpu.VMEM((2 * REACH + 1, BOND, CW), jnp.bfloat16)
    return pl.pallas_call(
        kernel,
        out_shape=jax.ShapeDtypeStruct((1, ROWS, LEFT), jnp.bfloat16),
        in_specs=[smem, smem, any_space, any_space, any_space, any_space],
        out_specs=pl.BlockSpec(memory_space=pltpu.VMEM),
        scratch_shapes=[
            pltpu.VMEM((PER, BOND, BOND), jnp.bfloat16),
            pltpu.VMEM((CHUNKS, BOND, PER * CW), jnp.bfloat16),
            pltpu.VMEM((LEFT, BOND), jnp.bfloat16),
            pltpu.VMEM((ROWS, LEFT), jnp.bfloat16),
            block, block, block, block, block, block,
            pltpu.VMEM((BOND, PER * CW), jnp.bfloat16),
            pltpu.VMEM((BOND, BOND), jnp.float32),
            pltpu.VMEM((STEPS, BOND, BOND), jnp.bfloat16),
            pltpu.VMEM((STEPS, OPS, ROWS, BOND), jnp.bfloat16),
            pltpu.SemaphoreType.DMA((STEPS, SEMS)),
            pltpu.SemaphoreType.DMA((STEPS, SEMS)),
            pltpu.SemaphoreType.DMA((STEPS, OPS)),
            pltpu.SemaphoreType.DMA((STEPS, OPS)),
            pltpu.SemaphoreType.DMA((3 + CHUNKS * PER,)),
        ],
        compiler_params=pltpu.CompilerParams(
            collective_id=0, has_side_effects=True, vmem_limit_bytes=62 * 1024 * 1024
        ),
        name="hamiltonian",
    )(offsets, sector_sizes, wavefunction, basis, left_ops, right_ops)


def solution(mesh):
    return jax.shard_map(
        on_device,
        mesh=mesh,
        in_specs=(
            P("sector", "op", None),
            P("sector", None, None),
            P("op", None, None),
            P("op", None, None),
            P("op"),
            P("sector"),
        ),
        out_specs=P("sector", "op", None),
        check_vma=False,
    )
```

```python
import functools

import jax
import jax.numpy as jnp
from jax import lax
from jax.experimental import pallas as pl
from jax.experimental.pallas import tpu as pltpu
from jax.sharding import PartitionSpec as P

BOND = 768
LEFT = 1536
REACH = 2
STEPS = 2
PER = 5
ROWS = 96
CW = 256
CHUNKS = BOND // CW
OPS = 8
increment_width = 0.75
MESH = pl.DeviceIdType.MESH
METHOD = ("B", "B", "N")
ORDER = (0, 2, 1)


def dot_nt(a, b):
    return lax.dot_general(
        a, b, (((1,), (1,)), ((), ())), preferred_element_type=jnp.float32
    )


def dot_nn(a, b):
    return jnp.dot(a, b, preferred_element_type=jnp.float32)


class Names:
    def __init__(self):
        self.index = {}

    def __call__(self, *key):
        return self.index.setdefault(key, len(self.index))


SEMS = 80


def kernel(
    off_ref, size_ref, wf_hbm, basis_hbm, left_hbm, right_hbm, out_ref,
    left, right, basis, cur, x00, x01, x02, x10, x11, x12,
    h, acc, rotated, gram, summed, part, arrived, send_sem, recv_sem, rs_send, rs_recv, load_sem,
):
    s = lax.axis_index("sector")
    o = lax.axis_index("op")
    x, zh = o // 2, lax.rem(o, 2)
    core = lax.rem(s, 2)
    chip = s // 2
    has_lo, has_hi = chip > 0, chip < 7
    cross_lo, cross_hi = chip == 4, chip == 3
    plain_lo, plain_hi = has_lo & (chip != 4), has_hi & (chip != 3)
    partner = s + 1 - 2 * core
    z_peer = x * 2 + (1 - zh)
    x_right = lax.rem(x + 1, 4)
    x_left = lax.rem(x + 3, 4)
    x_far = lax.rem(x + 2, 4)
    op_right, op_left = x_right * 2 + zh, x_left * 2 + zh

    loads = {}

    def load(name, src, dst, i):
        cp = pltpu.make_async_copy(src, dst, load_sem.at[i])
        cp.start()
        loads[name] = cp

    load("wf", wf_hbm.at[0], cur, 0)
    load("basis", basis_hbm.at[0], basis, 1)

    barrier = pltpu.get_barrier_semaphore()
    for j in range(1, OPS):
        pl.semaphore_signal(
            barrier, inc=1, device_id={"sector": s, "op": lax.rem(o + j, OPS)}, device_id_type=MESH
        )
    pl.semaphore_signal(barrier, inc=1, device_id={"sector": partner, "op": o}, device_id_type=MESH)

    @pl.when(has_lo)
    def _():
        pl.semaphore_signal(barrier, inc=1, device_id={"sector": s - 2, "op": o}, device_id_type=MESH)

    @pl.when(has_hi)
    def _():
        pl.semaphore_signal(barrier, inc=1, device_id={"sector": s + 2, "op": o}, device_id_type=MESH)

    load("left", left_hbm, left, 2)
    for c in range(CHUNKS):
        for k in range(PER):
            span = slice(c * CW, (c + 1) * CW)
            load(
                ("right", c, k), right_hbm.at[k, :, span], right.at[c, :, k * CW : (k + 1) * CW],
                3 + c * PER + k,
            )

    xg = ((x00, x01, x02), (x10, x11, x12))

    def blank(bufs):
        for buf in bufs:
            @pl.when(jnp.logical_not(has_lo))
            def _():
                buf[0] = jnp.zeros((BOND, CW), jnp.bfloat16)

            @pl.when(jnp.logical_not(has_lo) & (core == 0))
            def _():
                buf[1] = jnp.zeros((BOND, CW), jnp.bfloat16)

            @pl.when(jnp.logical_not(has_hi))
            def _():
                buf[4] = jnp.zeros((BOND, CW), jnp.bfloat16)

            @pl.when(jnp.logical_not(has_hi) & (core == 1))
            def _():
                buf[3] = jnp.zeros((BOND, CW), jnp.bfloat16)

    columns = lax.broadcasted_iota(jnp.int32, (ROWS, LEFT), 1)
    live = columns < size_ref[0]
    loads["wf"].wait()
    cur[...] = jnp.where(live, cur[...], jnp.zeros((ROWS, LEFT), jnp.bfloat16))
    loads["basis"].wait()

    def rows_of(start, count):
        return pl.ds(pl.multiple_of(start, ROWS), count)

    own_rows = rows_of(o * ROWS, ROWS)
    z_rows = rows_of(z_peer * ROWS, ROWS)
    pair_rows = rows_of(x * 192, 192)
    left_pair = rows_of(x_left * 192, 192)
    right_pair = rows_of(x_right * 192, 192)
    far_pair = rows_of(x_far * 192, 192)
    lo_half = lambda px: rows_of(px * 192, ROWS)
    hi_half = lambda px: rows_of(px * 192 + ROWS, ROWS)

    def lift(target):
        lifted = dot_nt(summed[...], basis[...])
        fresh = cur[...].astype(jnp.float32) - increment_width * lifted
        target[...] = fresh.astype(jnp.bfloat16)

    for step in range(STEPS):
        names = Names()
        waits = []
        bufs = xg[step]

        def send(key, src, dst, sector, op, when=None):
            i = names(*key)

            def copy():
                return pltpu.make_async_remote_copy(
                    src_ref=src, dst_ref=dst,
                    send_sem=send_sem.at[step, i], recv_sem=recv_sem.at[step, i],
                    device_id={"sector": sector, "op": op}, device_id_type=MESH,
                )

            if when is None:
                copy().start()
            else:
                @pl.when(when)
                def _():
                    copy().start()
            waits.append((copy, when))

        def arrive(key, dst, when=None):
            i = names(*key)

            def body():
                pltpu.make_async_remote_copy(
                    src_ref=dst, dst_ref=dst,
                    send_sem=send_sem.at[step, i], recv_sem=recv_sem.at[step, i],
                    device_id={"sector": partner, "op": o}, device_id_type=MESH,
                ).wait_recv()

            if when is None:
                body()
            else:
                pl.when(when)(body)

        def slot_when(slot):
            return {0: has_lo, 2: None, 4: has_hi}[slot]

        def send_y(ch, rows, name, up=has_hi, down=has_lo):
            buf = bufs[ch]
            send((ch, "y-up", name), buf.at[2, rows], buf.at[0, rows], s + 2, o, up)
            send((ch, "y-dn", name), buf.at[2, rows], buf.at[4, rows], s - 2, o, down)

        def arrive_y(ch, rows, name):
            buf = bufs[ch]
            arrive((ch, "y-up", name), buf.at[0, rows], has_lo)
            arrive((ch, "y-dn", name), buf.at[4, rows], has_hi)

        def gather_z(ch, slot):
            buf = bufs[ch]
            send((ch, slot, "z"), buf.at[slot, own_rows], buf.at[slot, own_rows], s, z_peer, slot_when(slot))

        def arrive_z(ch, slot):
            arrive((ch, slot, "z"), bufs[ch].at[slot, z_rows], slot_when(slot))

        def gather_x(ch, slot):
            buf = bufs[ch]
            pair = buf.at[slot, pair_rows]
            send((ch, slot, "right"), pair, pair, s, op_right, slot_when(slot))
            send((ch, slot, "left"), pair, pair, s, op_left, slot_when(slot))

        def relay_x(ch, slot):
            buf = bufs[ch]
            arrive((ch, slot, "right"), buf.at[slot, left_pair], slot_when(slot))
            half = buf.at[slot, lo_half(x_left)]
            send((ch, slot, "right2"), half, half, s, op_right, slot_when(slot))
            arrive((ch, slot, "left"), buf.at[slot, right_pair], slot_when(slot))
            half = buf.at[slot, hi_half(x_right)]
            send((ch, slot, "left2"), half, half, s, op_left, slot_when(slot))

        def finish_x(ch, slot):
            buf = bufs[ch]
            arrive((ch, slot, "right2"), buf.at[slot, lo_half(x_far)], slot_when(slot))
            arrive((ch, slot, "left2"), buf.at[slot, hi_half(x_far)], slot_when(slot))

        def own_across(ch):
            buf = bufs[ch]
            send((ch, "own"), buf.at[2], buf.at[1 + 2 * core], partner, o)

        def far_across(ch):
            buf = bufs[ch]
            there = ((core == 0) & has_hi) | ((core == 1) & has_lo)
            send((ch, "far"), buf.at[4 - 4 * core], buf.at[3 - 2 * core], partner, o, there)

        def arrive_across(ch):
            buf = bufs[ch]
            here = ((core == 0) & has_lo) | ((core == 1) & has_hi)
            arrive((ch, "own"), buf.at[3 - 2 * core])
            arrive((ch, "far"), buf.at[1 + 2 * core], here)

        def halves(ch):
            buf = bufs[ch]

            def body(k, carry):
                d = off_ref[k] + REACH
                span = pl.ds(pl.multiple_of(k * CW, CW), CW)
                h[:, span] = dot_nn(left[k], buf[d]).astype(jnp.bfloat16)
                return carry

            lax.fori_loop(0, PER, body, 0, unroll=True)

        def second(ch, rows):
            return dot_nt(h[rows], right[ch])

        def accumulate(ch, first):
            rows = slice(None)
            if first:
                acc[...] = second(ch, rows)
            else:
                acc[...] += second(ch, rows)

        def rotate(ch):
            span = slice(ch * CW, (ch + 1) * CW)
            if step == 0:
                rows = dot_nn(cur[...], basis[:, span])
                rotated[:, span] = rows
            else:
                rows = rotated[:, span] - increment_width * dot_nn(summed[...], gram[:, span])
            bufs[ch][2, own_rows] = rows.astype(jnp.bfloat16)

        def bring(ch):
            if METHOD[ch] == "B":
                arrive_y(ch, pair_rows, "pair")
                arrive_y(ch, left_pair, "left")
                arrive_y(ch, right_pair, "right")
                arrive_y(ch, far_pair, "far")
            else:
                finish_x(ch, 0)
                finish_x(ch, 4)
            far_across(ch)

        a, b, d = 0, 1, 2
        rotate(a)
        if step == 0:
            pl.semaphore_wait(
                barrier, OPS + has_lo.astype(jnp.int32) + has_hi.astype(jnp.int32)
            )
        gather_z(a, 2)
        rotate(d)
        gather_z(d, 2)
        rotate(b)
        gather_z(b, 2)
        if step == 0:
            blank(xg[0])
            blank(xg[1])
        arrive_z(a, 2)
        gather_x(a, 2)
        send_y(a, pair_rows, "pair", plain_hi, plain_lo)
        arrive_z(d, 2)
        send_y(d, pair_rows, "pair")
        arrive_z(b, 2)
        gather_x(b, 2)
        gather_x(d, 2)
        relay_x(a, 2)
        send_y(a, pair_rows, "pair", cross_hi, cross_lo)
        send_y(a, left_pair, "left")
        send_y(a, right_pair, "right")
        arrive_y(d, pair_rows, "pair")
        gather_x(d, 0)
        gather_x(d, 4)
        relay_x(b, 2)
        finish_x(a, 2)
        send_y(a, far_pair, "far")
        own_across(a)
        send_y(b, pair_rows, "pair")
        send_y(b, left_pair, "left")
        send_y(b, right_pair, "right")
        relay_x(d, 2)
        finish_x(b, 2)
        send_y(b, far_pair, "far")
        own_across(b)
        finish_x(d, 2)
        own_across(d)
        relay_x(d, 0)
        relay_x(d, 4)

        if step == 0:
            loads["left"].wait()
            for c in range(CHUNKS):
                for k in range(PER):
                    loads["right", c, k].wait()

        bring(a)
        arrive_across(a)
        halves(a)
        accumulate(a, True)
        bring(d)
        arrive_across(d)
        halves(d)
        bring(b)
        accumulate(d, False)
        arrive_across(b)
        halves(b)
        last = ORDER[-1]
        rs_waits = []
        for i in range(2):
            half = lax.rem(x // 2 + 1 + i, 2)
            rows = pl.ds(pl.multiple_of(half * 384, 384), 384)
            part[step, rows] = (acc[rows] + second(last, rows)).astype(jnp.bfloat16)
            for j in (((1, 3, 2, 0), (1, 3, 2)))[i]:
                peer = half * 4 + lax.rem(lax.rem(o, 4) + j, 4)
                peer_rows = rows_of(peer * ROWS, ROWS)

                def copy(peer=peer, peer_rows=peer_rows):
                    return pltpu.make_async_remote_copy(
                        src_ref=part.at[step, peer_rows], dst_ref=arrived.at[step, o],
                        send_sem=rs_send.at[step, peer], recv_sem=rs_recv.at[step, o],
                        device_id={"sector": s, "op": peer}, device_id_type=MESH,
                    )

                if i == 1 and j == 0:
                    continue
                copy().start()
                rs_waits.append(copy)

        if step == 0:
            basis[...] = jnp.where(
                lax.broadcasted_iota(jnp.int32, (LEFT, BOND), 0) < size_ref[0],
                basis[...], jnp.zeros((LEFT, BOND), jnp.bfloat16),
            )
            gram[...] = lax.dot_general(
                basis[...], basis[...], (((0,), (0,)), ((), ())),
                preferred_element_type=jnp.float32,
            ).astype(jnp.bfloat16)
        else:
            lift(cur)
        total = part[step, own_rows].astype(jnp.float32)
        for j in range(1, OPS):
            peer = lax.rem(o + j, OPS)
            pltpu.make_async_remote_copy(
                src_ref=arrived.at[step, peer], dst_ref=arrived.at[step, peer],
                send_sem=rs_send.at[step, peer], recv_sem=rs_recv.at[step, peer],
                device_id={"sector": s, "op": peer}, device_id_type=MESH,
            ).wait_recv()
            total = total + arrived[step, peer].astype(jnp.float32)
        summed[...] = total.astype(jnp.bfloat16)
        if step == STEPS - 1:
            lift(out_ref.at[0])
        for copy in rs_waits:
            copy().wait_send()
        for copy, when in waits:
            if when is None:
                copy().wait_send()
            else:
                @pl.when(when)
                def _():
                    copy().wait_send()
        assert len(names.index) <= SEMS


def on_device(wavefunction, basis, left_ops, right_ops, offsets, sector_sizes):
    any_space = pl.BlockSpec(memory_space=pl.ANY)
    smem = pl.BlockSpec(memory_space=pltpu.SMEM)
    block = pltpu.VMEM((2 * REACH + 1, BOND, CW), jnp.bfloat16)
    return pl.pallas_call(
        kernel,
        out_shape=jax.ShapeDtypeStruct((1, ROWS, LEFT), jnp.bfloat16),
        in_specs=[smem, smem, any_space, any_space, any_space, any_space],
        out_specs=pl.BlockSpec(memory_space=pltpu.VMEM),
        scratch_shapes=[
            pltpu.VMEM((PER, BOND, BOND), jnp.bfloat16),
            pltpu.VMEM((CHUNKS, BOND, PER * CW), jnp.bfloat16),
            pltpu.VMEM((LEFT, BOND), jnp.bfloat16),
            pltpu.VMEM((ROWS, LEFT), jnp.bfloat16),
            block, block, block, block, block, block,
            pltpu.VMEM((BOND, PER * CW), jnp.bfloat16),
            pltpu.VMEM((BOND, BOND), jnp.float32),
            pltpu.VMEM((ROWS, BOND), jnp.float32),
            pltpu.VMEM((BOND, BOND), jnp.bfloat16),
            pltpu.VMEM((ROWS, BOND), jnp.bfloat16),
            pltpu.VMEM((STEPS, BOND, BOND), jnp.bfloat16),
            pltpu.VMEM((STEPS, OPS, ROWS, BOND), jnp.bfloat16),
            pltpu.SemaphoreType.DMA((STEPS, SEMS)),
            pltpu.SemaphoreType.DMA((STEPS, SEMS)),
            pltpu.SemaphoreType.DMA((STEPS, OPS)),
            pltpu.SemaphoreType.DMA((STEPS, OPS)),
            pltpu.SemaphoreType.DMA((3 + CHUNKS * PER,)),
        ],
        compiler_params=pltpu.CompilerParams(
            collective_id=0, has_side_effects=True, vmem_limit_bytes=62 * 1024 * 1024
        ),
        name="hamiltonian",
    )(offsets, sector_sizes, wavefunction, basis, left_ops, right_ops)


def solution(mesh):
    return jax.shard_map(
        on_device,
        mesh=mesh,
        in_specs=(
            P("sector", "op", None),
            P("sector", None, None),
            P("op", None, None),
            P("op", None, None),
            P("op"),
            P("sector"),
        ),
        out_specs=P("sector", "op", None),
        check_vma=False,
    )
```

```python
import functools

import jax
import jax.numpy as jnp
from jax import lax
from jax.experimental import pallas as pl
from jax.experimental.pallas import tpu as pltpu
from jax.sharding import PartitionSpec as P

BOND = 768
LEFT = 1536
REACH = 2
STEPS = 2
PER = 5
ROWS = 96
CW = 256
CHUNKS = BOND // CW
OPS = 8
increment_width = 0.75
MESH = pl.DeviceIdType.MESH
METHOD = ("B", "B", "N")
ORDER = (0, 2, 1)


def dot_nt(a, b):
    return lax.dot_general(
        a, b, (((1,), (1,)), ((), ())), preferred_element_type=jnp.float32
    )


def dot_nn(a, b):
    return jnp.dot(a, b, preferred_element_type=jnp.float32)


class Names:
    def __init__(self):
        self.index = {}

    def __call__(self, *key):
        return self.index.setdefault(key, len(self.index))


SEMS = 80


def kernel(
    off_ref, size_ref, wf_hbm, basis_hbm, left_hbm, right_hbm, out_ref,
    left, right, basis, cur, x00, x01, x02, x10, x11, x12,
    h, acc, rotated, gram, summed, part, arrived, send_sem, recv_sem, rs_send, rs_recv, load_sem,
):
    s = lax.axis_index("sector")
    o = lax.axis_index("op")
    x, zh = o // 2, lax.rem(o, 2)
    core = lax.rem(s, 2)
    chip = s // 2
    has_lo, has_hi = chip > 0, chip < 7
    cross_lo, cross_hi = chip == 4, chip == 3
    plain_lo, plain_hi = has_lo & (chip != 4), has_hi & (chip != 3)
    partner = s + 1 - 2 * core
    z_peer = x * 2 + (1 - zh)
    x_right = lax.rem(x + 1, 4)
    x_left = lax.rem(x + 3, 4)
    x_far = lax.rem(x + 2, 4)
    op_right, op_left = x_right * 2 + zh, x_left * 2 + zh

    loads = {}

    def load(name, src, dst, i):
        cp = pltpu.make_async_copy(src, dst, load_sem.at[i])
        cp.start()
        loads[name] = cp

    load("wf", wf_hbm.at[0], cur, 0)
    load("basis", basis_hbm.at[0], basis, 1)

    barrier = pltpu.get_barrier_semaphore()
    for j in range(1, OPS):
        pl.semaphore_signal(
            barrier, inc=1, device_id={"sector": s, "op": lax.rem(o + j, OPS)}, device_id_type=MESH
        )
    pl.semaphore_signal(barrier, inc=1, device_id={"sector": partner, "op": o}, device_id_type=MESH)

    @pl.when(has_lo)
    def _():
        pl.semaphore_signal(barrier, inc=1, device_id={"sector": s - 2, "op": o}, device_id_type=MESH)

    @pl.when(has_hi)
    def _():
        pl.semaphore_signal(barrier, inc=1, device_id={"sector": s + 2, "op": o}, device_id_type=MESH)

    load("left", left_hbm, left, 2)
    for c in range(CHUNKS):
        for k in range(PER):
            span = slice(c * CW, (c + 1) * CW)
            load(
                ("right", c, k), right_hbm.at[k, :, span], right.at[c, :, k * CW : (k + 1) * CW],
                3 + c * PER + k,
            )

    xg = ((x00, x01, x02), (x10, x11, x12))

    def blank(bufs):
        for buf in bufs:
            @pl.when(jnp.logical_not(has_lo))
            def _():
                buf[0] = jnp.zeros((BOND, CW), jnp.bfloat16)

            @pl.when(jnp.logical_not(has_lo) & (core == 0))
            def _():
                buf[1] = jnp.zeros((BOND, CW), jnp.bfloat16)

            @pl.when(jnp.logical_not(has_hi))
            def _():
                buf[4] = jnp.zeros((BOND, CW), jnp.bfloat16)

            @pl.when(jnp.logical_not(has_hi) & (core == 1))
            def _():
                buf[3] = jnp.zeros((BOND, CW), jnp.bfloat16)

    columns = lax.broadcasted_iota(jnp.int32, (ROWS, LEFT), 1)
    live = columns < size_ref[0]
    loads["wf"].wait()
    cur[...] = jnp.where(live, cur[...], jnp.zeros((ROWS, LEFT), jnp.bfloat16))
    loads["basis"].wait()

    def rows_of(start, count):
        return pl.ds(pl.multiple_of(start, ROWS), count)

    own_rows = rows_of(o * ROWS, ROWS)
    z_rows = rows_of(z_peer * ROWS, ROWS)
    pair_rows = rows_of(x * 192, 192)
    left_pair = rows_of(x_left * 192, 192)
    right_pair = rows_of(x_right * 192, 192)
    far_pair = rows_of(x_far * 192, 192)
    lo_half = lambda px: rows_of(px * 192, ROWS)
    hi_half = lambda px: rows_of(px * 192 + ROWS, ROWS)

    def lift(target):
        lifted = dot_nt(summed[...], basis[...])
        fresh = cur[...].astype(jnp.float32) - increment_width * lifted
        target[...] = fresh.astype(jnp.bfloat16)

    for step in range(STEPS):
        names = Names()
        waits = []
        bufs = xg[step]

        def send(key, src, dst, sector, op, when=None):
            i = names(*key)

            def copy():
                return pltpu.make_async_remote_copy(
                    src_ref=src, dst_ref=dst,
                    send_sem=send_sem.at[step, i], recv_sem=recv_sem.at[step, i],
                    device_id={"sector": sector, "op": op}, device_id_type=MESH,
                )

            if when is None:
                copy().start()
            else:
                @pl.when(when)
                def _():
                    copy().start()
            waits.append((copy, when))

        def arrive(key, dst, when=None):
            i = names(*key)

            def body():
                pltpu.make_async_remote_copy(
                    src_ref=dst, dst_ref=dst,
                    send_sem=send_sem.at[step, i], recv_sem=recv_sem.at[step, i],
                    device_id={"sector": partner, "op": o}, device_id_type=MESH,
                ).wait_recv()

            if when is None:
                body()
            else:
                pl.when(when)(body)

        def slot_when(slot):
            return {0: has_lo, 2: None, 4: has_hi}[slot]

        def send_y(ch, rows, name, up=has_hi, down=has_lo):
            buf = bufs[ch]
            send((ch, "y-up", name), buf.at[2, rows], buf.at[0, rows], s + 2, o, up)
            send((ch, "y-dn", name), buf.at[2, rows], buf.at[4, rows], s - 2, o, down)

        def arrive_y(ch, rows, name):
            buf = bufs[ch]
            arrive((ch, "y-up", name), buf.at[0, rows], has_lo)
            arrive((ch, "y-dn", name), buf.at[4, rows], has_hi)

        def gather_z(ch, slot):
            buf = bufs[ch]
            send((ch, slot, "z"), buf.at[slot, own_rows], buf.at[slot, own_rows], s, z_peer, slot_when(slot))

        def arrive_z(ch, slot):
            arrive((ch, slot, "z"), bufs[ch].at[slot, z_rows], slot_when(slot))

        def gather_x(ch, slot):
            buf = bufs[ch]
            pair = buf.at[slot, pair_rows]
            send((ch, slot, "right"), pair, pair, s, op_right, slot_when(slot))
            send((ch, slot, "left"), pair, pair, s, op_left, slot_when(slot))

        def relay_x(ch, slot):
            buf = bufs[ch]
            arrive((ch, slot, "right"), buf.at[slot, left_pair], slot_when(slot))
            half = buf.at[slot, lo_half(x_left)]
            send((ch, slot, "right2"), half, half, s, op_right, slot_when(slot))
            arrive((ch, slot, "left"), buf.at[slot, right_pair], slot_when(slot))
            half = buf.at[slot, hi_half(x_right)]
            send((ch, slot, "left2"), half, half, s, op_left, slot_when(slot))

        def finish_x(ch, slot):
            buf = bufs[ch]
            arrive((ch, slot, "right2"), buf.at[slot, lo_half(x_far)], slot_when(slot))
            arrive((ch, slot, "left2"), buf.at[slot, hi_half(x_far)], slot_when(slot))

        def own_across(ch):
            buf = bufs[ch]
            send((ch, "own"), buf.at[2], buf.at[1 + 2 * core], partner, o)

        def far_across(ch):
            buf = bufs[ch]
            there = ((core == 0) & has_hi) | ((core == 1) & has_lo)
            send((ch, "far"), buf.at[4 - 4 * core], buf.at[3 - 2 * core], partner, o, there)

        def arrive_across(ch):
            buf = bufs[ch]
            here = ((core == 0) & has_lo) | ((core == 1) & has_hi)
            arrive((ch, "own"), buf.at[3 - 2 * core])
            arrive((ch, "far"), buf.at[1 + 2 * core], here)

        def halves(ch):
            buf = bufs[ch]

            def body(k, carry):
                d = off_ref[k] + REACH
                span = pl.ds(pl.multiple_of(k * CW, CW), CW)
                h[:, span] = dot_nn(left[k], buf[d]).astype(jnp.bfloat16)
                return carry

            lax.fori_loop(0, PER, body, 0, unroll=True)

        def second(ch, rows):
            return dot_nt(h[rows], right[ch])

        def accumulate(ch, first):
            rows = slice(None)
            if first:
                acc[...] = second(ch, rows)
            else:
                acc[...] += second(ch, rows)

        def rotate(ch):
            span = slice(ch * CW, (ch + 1) * CW)
            if step == 0:
                rows = dot_nn(cur[...], basis[:, span])
                rotated[:, span] = rows
            else:
                rows = rotated[:, span] - increment_width * dot_nn(summed[...], gram[:, span])
            bufs[ch][2, own_rows] = rows.astype(jnp.bfloat16)

        def bring(ch):
            if METHOD[ch] == "B":
                arrive_y(ch, pair_rows, "pair")
                arrive_y(ch, left_pair, "left")
                arrive_y(ch, right_pair, "right")
                arrive_y(ch, far_pair, "far")
            else:
                finish_x(ch, 0)
                finish_x(ch, 4)
            far_across(ch)

        a, b, d = 0, 1, 2
        rotate(a)
        if step == 0:
            pl.semaphore_wait(
                barrier, OPS + has_lo.astype(jnp.int32) + has_hi.astype(jnp.int32)
            )
        gather_z(a, 2)
        rotate(d)
        gather_z(d, 2)
        rotate(b)
        gather_z(b, 2)
        if step == 0:
            blank(xg[0])
            blank(xg[1])
        arrive_z(a, 2)
        gather_x(a, 2)
        send_y(a, pair_rows, "pair", plain_hi, plain_lo)
        arrive_z(d, 2)
        send_y(d, pair_rows, "pair")
        arrive_z(b, 2)
        gather_x(b, 2)
        gather_x(d, 2)
        relay_x(a, 2)
        send_y(a, pair_rows, "pair", cross_hi, cross_lo)
        send_y(a, left_pair, "left")
        send_y(a, right_pair, "right")
        arrive_y(d, pair_rows, "pair")
        gather_x(d, 0)
        gather_x(d, 4)
        relay_x(b, 2)
        finish_x(a, 2)
        send_y(a, far_pair, "far")
        own_across(a)
        send_y(b, pair_rows, "pair")
        send_y(b, left_pair, "left")
        send_y(b, right_pair, "right")
        relay_x(d, 2)
        finish_x(b, 2)
        send_y(b, far_pair, "far")
        own_across(b)
        finish_x(d, 2)
        own_across(d)
        relay_x(d, 0)
        relay_x(d, 4)

        if step == 0:
            loads["left"].wait()
            for c in range(CHUNKS):
                for k in range(PER):
                    loads["right", c, k].wait()

        bring(a)
        arrive_across(a)
        halves(a)
        accumulate(a, True)
        bring(d)
        arrive_across(d)
        halves(d)
        bring(b)
        accumulate(d, False)
        arrive_across(b)
        halves(b)
        last = ORDER[-1]
        rs_waits = []
        for i in range(2):
            half = lax.rem(x // 2 + 1 + i, 2)
            rows = pl.ds(pl.multiple_of(half * 384, 384), 384)
            part[step, rows] = (acc[rows] + second(last, rows)).astype(jnp.bfloat16)
            for j in (((1, 3, 0, 2), (1, 3, 2)))[i]:
                peer = half * 4 + lax.rem(lax.rem(o, 4) + j, 4)
                peer_rows = rows_of(peer * ROWS, ROWS)

                def copy(peer=peer, peer_rows=peer_rows):
                    return pltpu.make_async_remote_copy(
                        src_ref=part.at[step, peer_rows], dst_ref=arrived.at[step, o],
                        send_sem=rs_send.at[step, peer], recv_sem=rs_recv.at[step, o],
                        device_id={"sector": s, "op": peer}, device_id_type=MESH,
                    )

                if i == 1 and j == 0:
                    continue
                copy().start()
                rs_waits.append(copy)

        if step == 0:
            basis[...] = jnp.where(
                lax.broadcasted_iota(jnp.int32, (LEFT, BOND), 0) < size_ref[0],
                basis[...], jnp.zeros((LEFT, BOND), jnp.bfloat16),
            )
            gram[...] = lax.dot_general(
                basis[...], basis[...], (((0,), (0,)), ((), ())),
                preferred_element_type=jnp.float32,
            ).astype(jnp.bfloat16)
        else:
            lift(cur)
        total = part[step, own_rows].astype(jnp.float32)
        for j in range(1, OPS):
            peer = lax.rem(o + j, OPS)
            pltpu.make_async_remote_copy(
                src_ref=arrived.at[step, peer], dst_ref=arrived.at[step, peer],
                send_sem=rs_send.at[step, peer], recv_sem=rs_recv.at[step, peer],
                device_id={"sector": s, "op": peer}, device_id_type=MESH,
            ).wait_recv()
            total = total + arrived[step, peer].astype(jnp.float32)
        summed[...] = total.astype(jnp.bfloat16)
        if step == STEPS - 1:
            lift(out_ref.at[0])
        for copy in rs_waits:
            copy().wait_send()
        for copy, when in waits:
            if when is None:
                copy().wait_send()
            else:
                @pl.when(when)
                def _():
                    copy().wait_send()
        assert len(names.index) <= SEMS


def on_device(wavefunction, basis, left_ops, right_ops, offsets, sector_sizes):
    any_space = pl.BlockSpec(memory_space=pl.ANY)
    smem = pl.BlockSpec(memory_space=pltpu.SMEM)
    block = pltpu.VMEM((2 * REACH + 1, BOND, CW), jnp.bfloat16)
    return pl.pallas_call(
        kernel,
        out_shape=jax.ShapeDtypeStruct((1, ROWS, LEFT), jnp.bfloat16),
        in_specs=[smem, smem, any_space, any_space, any_space, any_space],
        out_specs=pl.BlockSpec(memory_space=pltpu.VMEM),
        scratch_shapes=[
            pltpu.VMEM((PER, BOND, BOND), jnp.bfloat16),
            pltpu.VMEM((CHUNKS, BOND, PER * CW), jnp.bfloat16),
            pltpu.VMEM((LEFT, BOND), jnp.bfloat16),
            pltpu.VMEM((ROWS, LEFT), jnp.bfloat16),
            block, block, block, block, block, block,
            pltpu.VMEM((BOND, PER * CW), jnp.bfloat16),
            pltpu.VMEM((BOND, BOND), jnp.float32),
            pltpu.VMEM((ROWS, BOND), jnp.float32),
            pltpu.VMEM((BOND, BOND), jnp.bfloat16),
            pltpu.VMEM((ROWS, BOND), jnp.bfloat16),
            pltpu.VMEM((STEPS, BOND, BOND), jnp.bfloat16),
            pltpu.VMEM((STEPS, OPS, ROWS, BOND), jnp.bfloat16),
            pltpu.SemaphoreType.DMA((STEPS, SEMS)),
            pltpu.SemaphoreType.DMA((STEPS, SEMS)),
            pltpu.SemaphoreType.DMA((STEPS, OPS)),
            pltpu.SemaphoreType.DMA((STEPS, OPS)),
            pltpu.SemaphoreType.DMA((3 + CHUNKS * PER,)),
        ],
        compiler_params=pltpu.CompilerParams(
            collective_id=0, has_side_effects=True, vmem_limit_bytes=62 * 1024 * 1024
        ),
        name="hamiltonian",
    )(offsets, sector_sizes, wavefunction, basis, left_ops, right_ops)


def solution(mesh):
    return jax.shard_map(
        on_device,
        mesh=mesh,
        in_specs=(
            P("sector", "op", None),
            P("sector", None, None),
            P("op", None, None),
            P("op", None, None),
            P("op"),
            P("sector"),
        ),
        out_specs=P("sector", "op", None),
        check_vma=False,
    )
```
